8 devices in a mesh: right: 2 (over z, y), left: 4 (over x, core).
Axes of the slice: x: 2, y: 2, z: 1, core: 2. Of those that a mesh axis runs over, the one named last changes fastest.
Arguments:
- psi_init: float32 [2048, 2, 2, 2048], P('left', None, None, 'right')
- env_left: float32 [2048, 3, 2048], P('left')
- env_right: float32 [2048, 3, 2048], P('right')
- mpo_pair: float32 [3, 3, 2, 2, 2, 2], replicated
Outputs:
- output 1: float32 [5], replicated
- output 2: float32 [5], replicated
- output 3: float32 [2048, 2, 2, 2048], P('left', None, None, 'right')
All inputs are finite; a program needn't handle non-finite values.
Results may differ from the reference program's by a relative error of at most 0.001.
Values sent between devices are 32-bit elements.
A program may use at most 1 GiB of HBM per device.

```python
import math
import jax
import jax.numpy as jnp
from jax import lax

PHYS_DIM = 2
MPO_DIM = 3
BOND_DIM = 2048
KRYLOV_STEPS = 5
PREC_MODE = lax.Precision.HIGHEST


def sym_env(env_key, bond_dim, mpo_dim):
    key_mat, key_shift = jax.random.split(env_key)
    gauss_mat = jax.random.normal(key_mat, (bond_dim, mpo_dim, bond_dim), jnp.float32)
    sym_part = (gauss_mat + jnp.transpose(gauss_mat, (2, 1, 0))) / math.sqrt(2.0 * bond_dim)
    diag_shift = jax.random.normal(key_shift, (mpo_dim,), jnp.float32)
    eye_mat = jnp.eye(bond_dim, dtype=jnp.float32)
    return sym_part + eye_mat[:, None, :] * diag_shift[None, :, None]


def sym_mpo(mpo_key, mpo_dim, phys_dim):
    key_mat, key_diag = jax.random.split(mpo_key)
    gauss_mat = jax.random.normal(key_mat, (mpo_dim, mpo_dim, phys_dim, phys_dim, phys_dim, phys_dim), jnp.float32)
    sym_part = (gauss_mat + jnp.transpose(gauss_mat, (0, 1, 4, 5, 2, 3))) / (math.sqrt(2.0) * mpo_dim * phys_dim)
    diag_coef = jax.random.normal(key_diag, (mpo_dim, mpo_dim), jnp.float32) / mpo_dim
    eye_phys = jnp.eye(phys_dim * phys_dim, dtype=jnp.float32).reshape(phys_dim, phys_dim, phys_dim, phys_dim)
    return sym_part + diag_coef[:, :, None, None, None, None] * eye_phys[None, None]


def setup_inputs(seed: int = 0) -> dict:
    base_key = jax.random.key(seed)
    key_psi, key_left, key_right, key_mpo = jax.random.split(base_key, 4)
    psi_init = jax.random.normal(key_psi, (BOND_DIM, PHYS_DIM, PHYS_DIM, BOND_DIM), jnp.float32)
    return {
        "psi_init": psi_init,
        "env_left": sym_env(key_left, BOND_DIM, MPO_DIM),
        "env_right": sym_env(key_right, BOND_DIM, MPO_DIM),
        "mpo_pair": sym_mpo(key_mpo, MPO_DIM, PHYS_DIM),
    }


def apply_ham(in_vec, env_left, env_right, mpo_pair):
    stage_one = jnp.einsum("alc,asub->lcsub", env_left, in_vec, precision=PREC_MODE)
    stage_two = jnp.einsum("lrsutv,lcsub->rtvcb", mpo_pair, stage_one, precision=PREC_MODE)
    return jnp.einsum("rtvcb,bre->ctve", stage_two, env_right, precision=PREC_MODE)


def project_out(krylov_basis, residual, coeffs):
    for vec_idx, basis_vec in enumerate(krylov_basis):
        residual = residual - coeffs[vec_idx] * basis_vec
    return residual


def reference(psi_init, env_left, env_right, mpo_pair):
    init_norm = jnp.sqrt(jnp.sum(psi_init * psi_init))
    krylov_basis = [psi_init / init_norm]
    alpha_list = []
    beta_list = []
    for step_idx in range(KRYLOV_STEPS):
        residual = apply_ham(krylov_basis[-1], env_left, env_right, mpo_pair)
        first_pass = jnp.stack([jnp.sum(basis_vec * residual) for basis_vec in krylov_basis])
        alpha_list.append(first_pass[-1])
        residual = project_out(krylov_basis, residual, first_pass)
        second_pass = jnp.stack([jnp.sum(basis_vec * residual) for basis_vec in krylov_basis])
        residual = project_out(krylov_basis, residual, second_pass)
        beta_val = jnp.sqrt(jnp.sum(residual * residual))
        beta_list.append(beta_val)
        krylov_basis.append(residual / beta_val)
    out_scale = math.sqrt(float(psi_init.size))
    return jnp.stack(alpha_list), jnp.stack(beta_list), krylov_basis[-1] * out_scale
```

```python
import functools
import math
import jax
import jax.numpy as jnp
from jax import lax
from jax.experimental import pallas as pl
from jax.experimental.pallas import tpu as pltpu
from jax.sharding import PartitionSpec as P

KRYLOV_STEPS = 5
LANES = 128
PHYS = 4
BONDS = 3
AHEAD = 2
VMEM_BYTES = 66 * 1000 * 1000
F32 = jnp.float32
BF16 = jnp.bfloat16
ANY = pl.BlockSpec(memory_space=pltpu.HBM)
IN_VMEM = pl.BlockSpec(memory_space=pltpu.VMEM)
IN_SMEM = pl.BlockSpec(memory_space=pltpu.SMEM)
MESH = pl.DeviceIdType.MESH


def split3(x):
    hi = x.astype(BF16)
    rest = x - hi.astype(F32)
    mid = rest.astype(BF16)
    return hi, mid, (rest - mid.astype(F32)).astype(BF16)


def dot6(lhs, rhs):
    def one(p, q):
        return jnp.dot(lhs(p), rhs(q), preferred_element_type=F32)

    return one(2, 0) + one(0, 2) + one(1, 1) + one(1, 0) + one(0, 1) + one(0, 0)


def barrier(peers):
    sem = pltpu.get_barrier_semaphore()
    for peer in peers:
        pl.semaphore_signal(sem, inc=1, device_id=peer, device_id_type=MESH)
    pl.semaphore_wait(sem, len(peers))


def params(collective_id=None):
    return pltpu.CompilerParams(
        collective_id=collective_id,
        has_side_effects=collective_id is not None,
        vmem_limit_bytes=VMEM_BYTES,
    )


def split_matrix(x):
    rows, cols = x.shape
    block = 128

    def body(x_ref, o_ref):
        for p, part in enumerate(split3(x_ref[...])):
            o_ref[p] = part

    return pl.pallas_call(
        body,
        grid=(rows // block,),
        out_shape=jax.ShapeDtypeStruct((3, rows, cols), BF16),
        in_specs=[pl.BlockSpec((block, cols), lambda i: (i, 0))],
        out_specs=pl.BlockSpec((3, block, cols), lambda i: (0, i, 0)),
        compiler_params=params(),
    )(x)


def first_body(
    u, inv, w, ls, t2o, vo, pb, xb, fb,
    lv, vfl, vfr, vsl, vsr, t1, t2b,
    ps, pr, xs, xr, fs, fr, lsem, lload, rload, vsem, tsem,
):
    n_chunks, na, cols = u.shape
    half = 2 * na
    left = lax.axis_index("left")
    x, core = left // 2, left % 2
    partner = {"left": 2 * x + 1 - core}
    across = {"left": 2 * (1 - x) + core}
    mine = pl.ds(pl.multiple_of(core * na, na), na)
    other = pl.ds(pl.multiple_of((1 - core) * na, na), na)
    near = pl.ds(pl.multiple_of(x * half, half), half)
    far = pl.ds(pl.multiple_of((1 - x) * half, half), half)

    def to_partner(k):
        return pltpu.make_async_remote_copy(u.at[k], pb.at[k], ps.at[k], pr.at[k], device_id=partner, device_id_type=MESH)

    def to_across(k):
        return pltpu.make_async_remote_copy(u.at[k], xb.at[k], xs.at[k], xr.at[k], device_id=across, device_id_type=MESH)

    def forward(k):
        return pltpu.make_async_remote_copy(xb.at[k], fb.at[k], fs.at[k], fr.at[k], device_id=partner, device_id_type=MESH)

    def load_l(p):
        return pltpu.make_async_copy(ls.at[p], lv.at[p], lsem.at[p])

    def load_mine(k):
        return pltpu.make_async_copy(u.at[k], vfl.at[k % 2, mine], lload.at[k % 2, 0])

    def load_partner(k):
        return pltpu.make_async_copy(pb.at[k], vfl.at[k % 2, other], lload.at[k % 2, 1])

    def load_across(k):
        return pltpu.make_async_copy(xb.at[k], vfr.at[mine], rload.at[0])

    def load_forward(k):
        return pltpu.make_async_copy(fb.at[k], vfr.at[other], rload.at[1])

    def store_v(k):
        return pltpu.make_async_copy(vfl.at[k % 2, mine], vo.at[k], vsem.at[k % 2])

    def store_t2(k):
        return pltpu.make_async_copy(t2b.at[k % 2], t2o.at[k], tsem.at[k % 2])

    barrier([partner, across])
    for k in range(n_chunks):
        to_across(k).start()
    for k in range(n_chunks):
        to_partner(k).start()
    load_mine(0).start()
    for p in range(3):
        load_l(p).start()
    to_partner(0).wait_recv()
    load_partner(0).start()
    scale = inv[0:1, 0:1]

    def split_half(src, dst, keep):
        block = 32

        @pl.loop(0, half // block)
        def _(i):
            rows = pl.ds(pl.multiple_of(i * block, block), block)
            v = src[rows, :] * scale
            if keep:
                src[rows, :] = v
            for p, part in enumerate(split3(v)):
                dst[p, rows, :] = part

    @pl.loop(0, n_chunks + AHEAD)
    def _(k):
        back = k - AHEAD

        @pl.when(back >= 0)
        def _():
            to_across(back).wait_recv()
            forward(back).start()
            load_across(back).start()

        @pl.when(k < n_chunks)
        def _():
            load_mine(k).wait()
            load_partner(k).wait()

            @pl.when(k + 1 < n_chunks)
            def _():
                @pl.when(k >= 1)
                def _():
                    store_v(k - 1).wait()

                load_mine(k + 1).start()
                to_partner(k + 1).wait_recv()
                load_partner(k + 1).start()

            split_half(vfl.at[k % 2], vsl, True)
            store_v(k).start()

            @pl.when(k == 0)
            def _():
                for p in range(3):
                    load_l(p).wait()

            @pl.loop(0, BONDS)
            def _(i):
                rows = pl.ds(pl.multiple_of(i * na, na), na)
                t1[k % (AHEAD + 1), rows, :] = dot6(lambda p: lv[p, rows, near], lambda q: vsl[q])

        @pl.when(back >= 0)
        def _():
            forward(back).wait_recv()
            load_forward(back).start()
            load_across(back).wait()
            load_forward(back).wait()
            split_half(vfr, vsr, False)
            slot = back % (AHEAD + 1)

            @pl.loop(0, BONDS)
            def _(i):
                rows = pl.ds(pl.multiple_of(i * na, na), na)
                t1[slot, rows, :] = t1[slot, rows, :] + dot6(lambda p: lv[p, rows, far], lambda q: vsr[q])

            @pl.when(back >= 2)
            def _():
                store_t2(back - 2).wait()

            block = 32

            @pl.loop(0, na // block)
            def _(i):
                base = pl.multiple_of(i * block, block)
                for r in range(BONDS):
                    for t in range(PHYS):
                        acc = None
                        for l in range(BONDS):
                            for s in range(PHYS):
                                term = w[((l * BONDS + r) * PHYS + s) * PHYS + t] * t1[slot, pl.ds(l * na + base, block), s * LANES : (s + 1) * LANES]
                                acc = term if acc is None else acc + term
                        for p, part in enumerate(split3(acc)):
                            t2b[back % 2, p, pl.ds(t * na + base, block), r * LANES : (r + 1) * LANES] = part

            store_t2(back).start()

    for k in range(max(n_chunks - 2, 0), n_chunks):
        store_v(k).wait()
        store_t2(k).wait()
    for k in range(n_chunks):
        to_across(k).wait_send()
        to_partner(k).wait_send()
        forward(k).wait_send()


def first(u, inv, w, ls, collective_id):
    n_chunks, na, cols = u.shape
    half = 2 * na
    vec = jax.ShapeDtypeStruct(u.shape, F32)
    dma = pltpu.SemaphoreType.DMA
    out = pl.pallas_call(
        first_body,
        out_shape=[jax.ShapeDtypeStruct((n_chunks, 3, PHYS * na, BONDS * LANES), BF16), vec, vec, vec, vec],
        in_specs=[ANY, IN_VMEM, IN_SMEM, ANY],
        out_specs=[ANY] * 5,
        scratch_shapes=[
            pltpu.VMEM(ls.shape, BF16),
            pltpu.VMEM((2, half, cols), F32),
            pltpu.VMEM((half, cols), F32),
            pltpu.VMEM((3, half, cols), BF16),
            pltpu.VMEM((3, half, cols), BF16),
            pltpu.VMEM((AHEAD + 1, BONDS * na, cols), F32),
            pltpu.VMEM((2, 3, PHYS * na, BONDS * LANES), BF16),
            *[dma((n_chunks,))] * 6,
            dma((3,)),
            dma((2, 2)),
            dma((2,)),
            dma((2,)),
            dma((2,)),
        ],
        compiler_params=params(collective_id),
        name="gather_first",
    )(u, inv, w, ls)
    return out[0], out[1]


def second_body(
    t2, rs, uo, sendb, recvb,
    rv, tv, ob, rb,
    ss, sr, rsem, tsem, stage, rload, osem,
):
    n_chunks, _, rows_all, k_chunk = t2.shape
    na = rows_all // PHYS
    _, k_all, wide = rv.shape[1:]
    mt = tv.shape[2]
    n_m = rows_all // mt
    per_t = na // mt
    n_n = rv.shape[0] // 2
    tiles = n_m * n_n
    per_chunk = wide // LANES
    right = lax.axis_index("right")
    peer = {"right": 1 - right}

    def load_r(h, n):
        owner = right if h else 1 - right
        col = pl.multiple_of((owner * n_n + n) * wide, wide)
        return pltpu.make_async_copy(rs.at[:, :, pl.ds(col, wide)], rv.at[h * n_n + n], rsem.at[h * n_n + n])

    def load_t(g):
        m, slot = g % n_m, g % 2
        rows = pl.ds(pl.multiple_of(m * mt, mt), mt)
        return [
            pltpu.make_async_copy(t2.at[c, :, rows], tv.at[slot, :, :, c * k_chunk : (c + 1) * k_chunk], tsem.at[slot, c])
            for c in range(n_chunks)
        ]

    def put(q):
        return pltpu.make_async_copy(ob.at[q % 3], sendb.at[q], stage.at[q % 3])

    def send(q):
        return pltpu.make_async_remote_copy(sendb.at[q], recvb.at[q], ss.at[q], sr.at[q], device_id=peer, device_id_type=MESH)

    def fetch(q):
        return pltpu.make_async_copy(recvb.at[q], rb.at[q % 2], rload.at[q % 2])

    def emit(q):
        m, n = q // n_n, q % n_n
        t, part = m // per_t, m % per_t
        rows = pl.ds(pl.multiple_of(part * mt, mt), mt)
        lanes = pl.ds(pl.multiple_of(t * LANES, LANES), LANES)
        return [
            pltpu.make_async_copy(
                ob.at[q % 3, :, c * LANES : (c + 1) * LANES],
                uo.at[n * per_chunk + c, rows, lanes],
                osem.at[q % 3, c],
            )
            for c in range(per_chunk)
        ]

    for copy in load_t(0):
        copy.start()
    for n in range(n_n):
        load_r(0, n).start()
    for n in range(n_n):
        load_r(1, n).start()
    barrier([peer])

    def tile(h, q, slot3):
        g = h * n_m + q // n_n

        @pl.when(q % n_n == 0)
        def _():
            for copy in load_t(g):
                copy.wait()

            @pl.when(g + 1 < 2 * n_m)
            def _():
                for copy in load_t(g + 1):
                    copy.start()

        for n in range(n_n):

            @pl.when(q == n)
            def _():
                load_r(h, n).wait()

        ob[slot3] = dot6(lambda p: tv[g % 2, p], lambda p: rv[h * n_n + q % n_n, p])

    @pl.loop(0, tiles)
    def _(q):
        @pl.when(q >= 1)
        def _():
            put(q - 1).wait()
            send(q - 1).start()

        tile(0, q, q % 3)
        put(q).start()

        @pl.when(q == 0)
        def _():
            pass

    put(tiles - 1).wait()
    send(tiles - 1).start()

    def finish(q):
        fetch(q).wait()
        ob[q % 3] = ob[q % 3] + rb[q % 2]
        for copy in emit(q):
            copy.start()

    @pl.loop(0, tiles)
    def _(q):
        @pl.when(q >= 1)
        def _():
            send(q - 1).wait_recv()
            fetch(q - 1).start()

        @pl.when(q >= 3)
        def _():
            for copy in emit(q - 3):
                copy.wait()

        tile(1, q, q % 3)

        @pl.when(q >= 1)
        def _():
            finish(q - 1)

    send(tiles - 1).wait_recv()
    fetch(tiles - 1).start()
    finish(tiles - 1)
    for q in range(max(tiles - 3, 0), tiles):
        for copy in emit(q):
            copy.wait()
    for q in range(tiles):
        send(q).wait_send()


def second(t2, rs, n_chunks, na, collective_id):
    _, k_all, nb = rs.shape
    wide = min(512, nb // 2)
    n_n = nb // 2 // wide
    mt = min(256, na)
    tiles = PHYS * na // mt * n_n
    per_chunk = wide // LANES
    dma = pltpu.SemaphoreType.DMA
    block = jax.ShapeDtypeStruct((tiles, mt, wide), F32)
    out = pl.pallas_call(
        second_body,
        out_shape=[jax.ShapeDtypeStruct((n_chunks, na, PHYS * LANES), F32), block, block],
        in_specs=[ANY, ANY],
        out_specs=[ANY] * 3,
        scratch_shapes=[
            pltpu.VMEM((2 * n_n, 3, k_all, wide), BF16),
            pltpu.VMEM((2, 3, mt, k_all), BF16),
            pltpu.VMEM((3, mt, wide), F32),
            pltpu.VMEM((2, mt, wide), F32),
            dma((tiles,)),
            dma((tiles,)),
            dma((2 * n_n,)),
            dma((2, n_chunks)),
            dma((3,)),
            dma((2,)),
            dma((3, per_chunk)),
        ],
        compiler_params=params(collective_id),
        name="second_scatter",
    )(t2, rs)
    return out[0]


def third_body(n_basis, n_right, n_left, *refs):
    u, *refs = refs
    vs, refs = refs[:n_basis], refs[n_basis:]
    if n_basis:
        uo, inv, alpha, beta, *refs = refs
    else:
        inv, *refs = refs
    ub, refs = refs[0], refs[1:]
    vb, refs = refs[:n_basis], refs[n_basis:]
    sbuf, rbuf, ssem, rsem, load, osem = refs
    n_chunks, na, cols = u.shape
    n_dev = n_right * n_left
    me = lax.axis_index("right") * n_left + lax.axis_index("left")
    block = 32

    def place(d):
        return {"right": d // n_left, "left": d % n_left}

    def loads(c):
        return [pltpu.make_async_copy(u.at[c], ub.at[c], load.at[0, c])] + [
            pltpu.make_async_copy(v.at[c], b.at[c], load.at[i + 1, c]) for i, (v, b) in enumerate(zip(vs, vb))
        ]

    for c in range(n_chunks):
        for copy in loads(c):
            copy.start()
    peers = [(me + k) % n_dev for k in range(1, n_dev)]
    barrier([place(d) for d in peers])

    def fold(x):
        return jnp.sum(x.reshape(block // 8, 8, cols), axis=0)

    def everywhere(step, sums):
        rows = [jnp.sum(jnp.sum(s.reshape(8, cols // LANES, LANES), axis=1), axis=0, keepdims=True) for s in sums]
        sbuf[step] = jnp.concatenate(rows + [jnp.zeros((8 - len(rows), LANES), F32)], axis=0)
        rbuf[step, me] = sbuf[step]

        def copy(k, to):
            return pltpu.make_async_remote_copy(
                sbuf.at[step], rbuf.at[step, to], ssem.at[step, k], rsem.at[step, to],
                device_id=place(peers[k]), device_id_type=MESH,
            )

        for k in range(n_dev - 1):
            copy(k, me).start()
        for k in range(n_dev - 1):
            copy(k, peers[k]).wait_recv()
        for k in range(n_dev - 1):
            copy(k, me).wait_send()
        total = rbuf[step, 0]
        for d in range(1, n_dev):
            total = total + rbuf[step, d]
        return [jnp.sum(total[i : i + 1, :]) for i in range(len(rows))]

    zero = jnp.zeros((8, cols), F32)

    def sweep(n_sums, per_block, before=None, after=None):
        @functools.partial(lax.fori_loop, 0, n_chunks, init_val=(zero,) * n_sums)
        def sums(c, carry):
            if before is not None:
                before(c)

            def inner(i, carry):
                rows = pl.ds(pl.multiple_of(i * block, block), block)
                return tuple(a + b for a, b in zip(carry, per_block(c, rows)))

            carry = lax.fori_loop(0, na // block, inner, carry)
            if after is not None:
                after(c)
            return carry

        return sums

    def arrive(c):
        for copy in loads(c):
            copy.wait()

    if not n_basis:
        def square(c, rows):
            x = ub[c, rows, :]
            return (fold(x * x),)

        (total,) = everywhere(0, sweep(1, square, before=arrive))
        inv[...] = 1.0 / jnp.sqrt(jnp.full((8, LANES), total, F32))
        return

    def overlaps(c, rows):
        x = ub[c, rows, :]
        return tuple(fold(b[c, rows, :] * x) for b in vb)

    once = everywhere(0, sweep(n_basis, overlaps, before=arrive))
    alpha[...] = jnp.full((8, LANES), once[-1], F32)

    def project(c, rows, coeffs):
        x = ub[c, rows, :]
        basis = [b[c, rows, :] for b in vb]
        for coeff, v in zip(coeffs, basis):
            x = x - coeff * v
        ub[c, rows, :] = x
        return x, basis

    def project_once(c, rows):
        x, basis = project(c, rows, once)
        return tuple(fold(v * x) for v in basis)

    twice = everywhere(1, sweep(n_basis, project_once))

    def project_twice(c, rows):
        x, _ = project(c, rows, twice)
        return (fold(x * x),)

    def store(c):
        return pltpu.make_async_copy(ub.at[c], uo.at[c], osem.at[c])

    (total,) = everywhere(2, sweep(1, project_twice, after=lambda c: store(c).start()))
    norm = jnp.sqrt(jnp.full((8, LANES), total, F32))
    beta[...] = norm
    inv[...] = 1.0 / norm
    for c in range(n_chunks):
        store(c).wait()


def third(u, basis, mesh, collective_id):
    n_chunks = u.shape[0]
    n_right, n_left = mesh.shape["right"], mesh.shape["left"]
    n_dev = n_right * n_left
    small = jax.ShapeDtypeStruct((8, LANES), F32)
    vec = jax.ShapeDtypeStruct(u.shape, F32)
    dma = pltpu.SemaphoreType.DMA
    return pl.pallas_call(
        functools.partial(third_body, len(basis), n_right, n_left),
        out_shape=[vec, small, small, small] if basis else [small],
        in_specs=[ANY] * (1 + len(basis)),
        out_specs=[ANY, IN_VMEM, IN_VMEM, IN_VMEM] if basis else [IN_VMEM],
        scratch_shapes=[
            *[pltpu.VMEM(u.shape, F32)] * (1 + len(basis)),
            pltpu.VMEM((3, 8, LANES), F32),
            pltpu.VMEM((3, n_dev, 8, LANES), F32),
            dma((3, n_dev)),
            dma((3, n_dev)),
            dma((1 + len(basis), n_chunks)),
            dma((n_chunks,)),
        ],
        compiler_params=params(collective_id),
        name="orthogonalise",
    )(u, *basis)


def solution(mesh):
    n_devices = mesh.shape["left"] * mesh.shape["right"]
    psi_spec = P("left", None, None, "right")

    def local_fn(psi_loc, env_left, env_right, mpo_pair):
        na, nbl = psi_loc.shape[0], psi_loc.shape[3]
        n_chunks = nbl // LANES
        ls = split_matrix(jnp.transpose(env_left, (1, 0, 2)).reshape(BONDS * na, -1))
        right_rows = env_right.reshape(n_chunks, LANES, BONDS, -1).transpose(0, 2, 1, 3)
        rs = split_matrix(right_rows.reshape(BONDS * nbl, -1))
        w = mpo_pair.reshape(-1)
        u = psi_loc.reshape(na, PHYS, n_chunks, LANES).transpose(2, 0, 1, 3).reshape(n_chunks, na, PHYS * LANES)
        (inv,) = third(u, [], mesh, 0)
        basis, alpha_list, beta_list = [], [], []
        for step_idx in range(KRYLOV_STEPS):
            t2, v = first(u, inv, w, ls, 3 * step_idx + 1)
            basis.append(v)
            hv = second(t2, rs, n_chunks, na, 3 * step_idx + 2)
            u, inv, alpha, beta = third(hv, basis, mesh, 3 * step_idx + 3)
            alpha_list.append(alpha[0, 0])
            beta_list.append(beta[0, 0])
        out_scale = math.sqrt(float(psi_loc.size * n_devices))
        last = u.reshape(n_chunks, na, PHYS, LANES).transpose(1, 2, 0, 3).reshape(psi_loc.shape)
        return jnp.stack(alpha_list), jnp.stack(beta_list), last * inv[0, 0] * out_scale

    return jax.shard_map(
        local_fn,
        mesh=mesh,
        in_specs=(psi_spec, P("left", None, None), P("right", None, None), P()),
        out_specs=(P(), P(), psi_spec),
        check_vma=False,
    )
```
